32 devices in a mesh: ctx: 8 (over z, x), tp: 4 (over y, core).
Axes of the slice: x: 2, y: 2, z: 4, core: 2. Of those that a mesh axis runs over, the one named last changes fastest.
Arguments:
- query_plain: bfloat16 [1024, 8192], P('ctx', 'tp'), may hold values from -6 to 6
- query_rotary: bfloat16 [1024, 4096], P('ctx', 'tp'), may hold values from -6 to 6
- latent_keys: bfloat16 [1024, 576], P(('ctx', 'tp')), may hold values from -100 to 100
- span_order: int32 [16], replicated, may hold values from 0 to 15, each once
- key_up: bfloat16 [64, 128, 512], P('tp'), may hold values from -0.5 to 0.5
- value_up: bfloat16 [64, 512, 128], P('tp'), may hold values from -0.5 to 0.5
- output_weight: bfloat16 [8192, 3584], P('tp'), may hold values from -0.125 to 0.125
Outputs:
- mixed: bfloat16 [1024, 3584], P('ctx', 'tp')
The draws below stay inside these ranges and needn't reach their ends.
Inputs may be any that keep to these rules, and one draw needn't show every extreme that they name: Stored rows s * 64 to (s + 1) * 64 - 1 are the tokens of span span_order[s] of the sequence, in order; each span appears once.
All inputs are finite; a program needn't handle non-finite values.
Results may differ from the reference program's by a relative error of at most 0.015.
Values may be sent and summed in bfloat16 or wider, within the bound.
A program may use at most 64 MiB of HBM per device.

```python
import math
import jax
import jax.numpy as jnp
from jax import lax

D = 3584
H = 64
NOPE = 128
ROPE = 64
LAT = 512
VD = 128
TOKENS = 1024
SPAN = 64
NCHUNK = 16


def draw_latent_keys(key, part):
    array_shape = (TOKENS, LAT + ROPE)
    values = jax.random.normal(jax.random.fold_in(key, 7), array_shape, jnp.float32)
    return jnp.clip(values, -6.0, 6.0).astype(jnp.bfloat16)


def block_levels(own_key, shape, cuts, smallest, high):
    def one(position, blocks):
        heights = jax.random.uniform(jax.random.fold_in(jax.random.fold_in(own_key, 6), position), (blocks,), jnp.float32, smallest / len(cuts), high / len(cuts))
        return jnp.repeat(jnp.exp(heights), shape[position] // blocks).reshape((-1,) + (1,) * (len(shape) - position - 1))

    factor_of = one(*cuts[0])
    for cut in cuts[1:]:
        factor_of = factor_of * one(*cut)
    return factor_of


def noise(key, shape, scale, reach, cuts=(), kind=jnp.bfloat16):
    result = scale * jax.random.normal(key, shape, jnp.float32)
    if cuts:
        result = result * block_levels(key, shape, cuts, -0.22, 0.18)
    return jnp.clip(result, -reach, reach).astype(kind)


def setup_inputs(seed: int = 0) -> dict:
    key_of = jax.random.split(jax.random.key(seed), 8)
    return {
        "query_plain": noise(key_of[0], (TOKENS, H * NOPE), 1.0, 6.0, ((0, 8), (1, 4))),
        "query_rotary": noise(key_of[1], (TOKENS, H * ROPE), 1.0, 6.0, ((0, 8), (1, 4))),
        "latent_keys": draw_latent_keys(jax.random.fold_in(key_of[7], 71), 0),
        "span_order": jax.random.permutation(key_of[3], NCHUNK).astype(jnp.int32),
        "key_up": noise(key_of[4], (H, NOPE, LAT), NOPE ** -0.5, 0.5, ((0, 4),)),
        "value_up": noise(key_of[5], (H, LAT, VD), (LAT // 4) ** -0.5, 0.5, ((0, 4),)),
        "output_weight": noise(key_of[6], (H * VD, D), (H * VD // 4) ** -0.5, 0.125, ((0, 4),)),
    }


rope_base = 10000.0

def rotate_pairs(values, places):
    halfway = values.shape[-1] // 2
    frequency = rope_base ** (-jnp.arange(halfway, dtype=jnp.float32) * 2.0 / values.shape[-1])
    angles = places.astype(jnp.float32)[:, None] * frequency[None, :]
    cosine = jnp.cos(angles)
    sine_part = jnp.sin(angles)
    first_half = values[..., :halfway]
    second_half = values[..., halfway:]
    return jnp.concatenate([first_half * cosine - second_half * sine_part, first_half * sine_part + second_half * cosine], axis=-1)

def reference(query_plain, query_rotary, latent_keys, span_order, key_up, value_up, output_weight):
    row_ids = jnp.arange(TOKENS, dtype=jnp.int32)
    places = (span_order[row_ids // SPAN] * SPAN + row_ids % SPAN).astype(jnp.int32)
    latent = latent_keys[:, :LAT]
    turned_keys = rotate_pairs(latent_keys[:, LAT:].astype(jnp.float32), places).astype(jnp.bfloat16)
    all_keys = jnp.concatenate([latent, turned_keys], axis=1)
    allowed = places[None, :] <= places[:, None]
    score_scale = 1.0 / math.sqrt(NOPE + ROPE)
    plain_heads = jnp.swapaxes(query_plain.reshape(TOKENS, H, NOPE), 0, 1)
    rotary_heads = jnp.swapaxes(query_rotary.reshape(TOKENS, H, ROPE), 0, 1)

    def one_head(inputs):
        head_plain, head_rotary, head_key_up, head_value_up = inputs
        absorbed = jnp.dot(head_plain, head_key_up, preferred_element_type=jnp.float32).astype(jnp.bfloat16)
        turned = rotate_pairs(head_rotary.astype(jnp.float32), places).astype(jnp.bfloat16)
        head_queries = jnp.concatenate([absorbed, turned], axis=1)
        scores = jnp.dot(head_queries, all_keys.T, preferred_element_type=jnp.float32) * score_scale
        highest = lax.optimization_barrier(jnp.max(jnp.where(allowed, scores, -jnp.inf), axis=1, keepdims=True))
        raised = jnp.where(allowed, jnp.exp(scores - highest), 0.0)
        weights = raised.astype(jnp.bfloat16)
        context = jnp.dot(weights, latent, preferred_element_type=jnp.float32) / lax.optimization_barrier(jnp.sum(raised, axis=1, keepdims=True))
        context = context.astype(jnp.bfloat16)
        return jnp.dot(context, head_value_up, preferred_element_type=jnp.float32).astype(jnp.bfloat16)
    head_out = lax.map(one_head, (plain_heads, rotary_heads, key_up, value_up))
    flat_out = jnp.swapaxes(head_out, 0, 1).reshape(TOKENS, H * VD)
    return jnp.dot(flat_out, output_weight, preferred_element_type=jnp.float32).astype(jnp.bfloat16)
```

```python
import math
from functools import partial

import jax
import jax.numpy as jnp
from jax import lax
from jax.experimental import pallas as pl
from jax.experimental.pallas import tpu as pltpu
from jax.sharding import PartitionSpec as P

rope_base = 10000.0
fill_score = -1e30
key_block_rows = 512


def rotate_pairs(values, places):
    halfway = values.shape[-1] // 2
    frequency = rope_base ** (-jnp.arange(halfway, dtype=jnp.float32) * 2.0 / values.shape[-1])
    angles = places.astype(jnp.float32)[:, None] * frequency[None, :]
    cosine = jnp.cos(angles)
    sine_part = jnp.sin(angles)
    if values.ndim == 3:
        cosine = cosine[:, None, :]
        sine_part = sine_part[:, None, :]
    first_half = values[..., :halfway]
    second_half = values[..., halfway:]
    return jnp.concatenate(
        [
            first_half * cosine - second_half * sine_part,
            first_half * sine_part + second_half * cosine,
        ],
        axis=-1,
    )


def token_places(span_table, indices, span_len):
    slot_ids = indices // span_len
    slot_table = jnp.arange(span_table.shape[0], dtype=jnp.int32)
    picked = jnp.sum(
        jnp.where(slot_ids[:, None] == slot_table[None, :], span_table[None, :], 0), axis=1
    )
    return picked * span_len + indices % span_len


def attend_block(
    carry_state, keys_block, key_places, queries, query_places, latent_width, score_scale
):
    running_max, running_sum, summed = carry_state
    scores = jnp.dot(queries, keys_block.T, preferred_element_type=jnp.float32) * score_scale
    allowed = key_places[None, :] <= query_places[:, None]
    masked = jnp.where(allowed, scores, fill_score)
    new_max = jnp.maximum(running_max, jnp.max(masked, axis=1))
    weights = jnp.where(allowed, jnp.exp(scores - new_max[:, None]), 0.0)
    factor = jnp.exp(running_max - new_max)
    new_sum = running_sum * factor + jnp.sum(weights, axis=1)
    new_summed = summed * factor[:, None] + jnp.dot(
        weights.astype(jnp.bfloat16),
        keys_block[:, :latent_width],
        preferred_element_type=jnp.float32,
    )
    return (new_max, new_sum, new_summed)


def attend_guarded(
    carry_state, keys_block, key_places, queries, query_places, latest, latent_width, score_scale
):
    return lax.cond(
        jnp.min(key_places) > latest,
        lambda carried: carried,
        lambda carried: attend_block(
            carried, keys_block, key_places, queries, query_places, latent_width, score_scale
        ),
        carry_state,
    )


def make_folder(queries, row_places, latest, span_order, span_len, latent_width, score_scale):

    def fold_piece(carry_state, key_piece, offset):
        piece_rows = key_piece.shape[0]
        key_places = token_places(span_order, jnp.arange(piece_rows, dtype=jnp.int32), span_len)

        def step_block(carried, block_parts):
            return (
                attend_guarded(
                    carried,
                    block_parts[0],
                    block_parts[1],
                    queries,
                    row_places,
                    latest,
                    latent_width,
                    score_scale,
                ),
                None,
            )

        stacked = key_piece.reshape(
            piece_rows // key_block_rows, key_block_rows, key_piece.shape[1]
        )
        stacked_places = key_places.reshape(piece_rows // key_block_rows, key_block_rows)
        result_state, unused = lax.scan(step_block, carry_state, (stacked, stacked_places))
        return result_state

    return fold_piece


def start_state(row_count, latent_width):
    return (
        jnp.full((row_count,), fill_score, jnp.float32),
        jnp.zeros((row_count,), jnp.float32),
        jnp.zeros((row_count,), jnp.float32)[:, None] + jnp.zeros((1, latent_width), jnp.float32),
    )


def project_out(final_state, token_count, head_count, latent_width, value_up, output_weight):
    running_max, running_sum, summed = final_state
    mixed_latent = (
        (summed / running_sum[:, None])
        .astype(jnp.bfloat16)
        .reshape(token_count, head_count, latent_width)
    )
    head_out = jnp.einsum(
        "thl,hlv->thv", mixed_latent, value_up, preferred_element_type=jnp.float32
    ).astype(jnp.bfloat16)
    head_out = head_out.reshape(token_count, head_count * value_up.shape[2])
    return jnp.dot(head_out, output_weight, preferred_element_type=jnp.float32)


def on_device(query_plain, query_rotary, latent_keys, span_order, key_up, value_up, output_weight):
    local_tokens = query_plain.shape[0]
    head_count = key_up.shape[0]
    plain_width = key_up.shape[1]
    latent_width = key_up.shape[2]
    rotary_width = query_rotary.shape[1] // head_count
    span_len = local_tokens // 2
    score_scale = 1.0 / math.sqrt(plain_width + rotary_width)
    first_row = lax.axis_index("ctx") * local_tokens
    query_places = token_places(
        span_order, first_row + jnp.arange(local_tokens, dtype=jnp.int32), span_len
    )
    absorbed = jnp.einsum(
        "thn,hnl->thl",
        query_plain.reshape(local_tokens, head_count, plain_width),
        key_up,
        preferred_element_type=jnp.float32,
    ).astype(jnp.bfloat16)
    turned = rotate_pairs(
        query_rotary.reshape(local_tokens, head_count, rotary_width).astype(jnp.float32),
        query_places,
    ).astype(jnp.bfloat16)
    queries = jnp.concatenate([absorbed, turned], axis=2).reshape(
        local_tokens * head_count, latent_width + rotary_width
    )
    row_places = jnp.repeat(query_places, head_count)
    own_rows = latent_keys.shape[0]
    own_first = first_row + lax.axis_index("tp") * own_rows
    own_places = token_places(
        span_order, own_first + jnp.arange(own_rows, dtype=jnp.int32), span_len
    )
    own_turned = rotate_pairs(latent_keys[:, latent_width:].astype(jnp.float32), own_places).astype(
        jnp.bfloat16
    )
    own_keys = jnp.concatenate([latent_keys[:, :latent_width], own_turned], axis=1)
    latest = jnp.max(query_places)
    folder = make_folder(
        queries, row_places, latest, span_order, span_len, latent_width, score_scale
    )
    group_keys = lax.all_gather(own_keys, "tp", axis=0, tiled=True)
    final_state = folder(
        start_state(local_tokens * head_count, latent_width),
        lax.all_gather(group_keys, "ctx", axis=0, tiled=True),
        jnp.int32(0),
    )
    head_terms = project_out(
        final_state, local_tokens, head_count, latent_width, value_up, output_weight
    )
    return lax.psum_scatter(head_terms.astype(jnp.bfloat16), "tp", scatter_dimension=1, tiled=True)


MESH = pl.DeviceIdType.MESH


def split_axes(mesh):
    ctx, tp = mesh.shape["ctx"], mesh.shape["tp"]
    x_size = 1
    while (2 * x_size) ** 2 <= ctx and ctx % (2 * x_size) == 0:
        x_size *= 2
    return ctx // x_size, x_size, tp // 2, 2


def fused_kernel(dims, span_len, latent, span_hbm, own_hbm, qp_hbm, qr_hbm, ku_hbm, vu_hbm, w_hbm,
                 out_ref, span_ref, own_ref, qp, qr, ku, vu, w, keys, queries, bias, scores, acc, top, total,
                 heads_out, own_part, sib_out, sib_in, y_out, y_in,
                 load_sem, zs, zr, ps, pr, ss, sr, rss, rsr, rys, ryr):
    Z, X, Y, C = dims
    ctx = lax.axis_index("ctx")
    tp = lax.axis_index("tp")
    z, x = ctx // X, ctx % X
    y, c = tp // C, tp % C
    R = own_ref.shape[0]
    rope = own_ref.shape[1] - latent
    T = qp.shape[0]
    H, plain = ku.shape[0], ku.shape[1]
    L = X * Y * C * R
    cols = out_ref.shape[1]
    scale = math.log2(math.e) / math.sqrt(plain + rope)

    def z_dev(zz):
        return (zz * X + x, tp)

    sibling = (ctx, y * C + (C - 1 - c))
    y_peer = (ctx, (1 - y) * C + c)
    plane_devs = [(z * X + 1 - x, tp), y_peer, (z * X + 1 - x, (1 - y) * C + c)]

    def plane_cols(kind):
        return [(x, y), (1 - x, y), (x, 1 - y), (1 - x, 1 - y)][kind]

    def z_order(i):
        low = i + (i >= z).astype(jnp.int32)
        high = Z - 1 - i - (i >= Z - 1 - z).astype(jnp.int32)
        return jnp.where(z < Z // 2, low, high)

    planes = [z] + [z_order(jnp.int32(i)) for i in range(Z - 1)]

    barrier = pltpu.get_barrier_semaphore()
    peers = [z_dev(zz) for zz in planes[1:]] + plane_devs + [sibling]
    for peer in peers:
        pl.semaphore_signal(barrier, inc=1, device_id=peer, device_id_type=MESH)

    loads = []
    pairs = ((own_hbm, own_ref), (span_hbm, span_ref), (qr_hbm, qr), (qp_hbm, qp), (ku_hbm, ku), (vu_hbm, vu), (w_hbm, w))
    for n, (src, dst) in enumerate(pairs):
        load = pltpu.make_async_copy(src, dst, load_sem.at[n])
        load.start()
        loads.append(load)

    lane = lax.broadcasted_iota(jnp.int32, (1, 128), 1)
    pair = lax.rem(lane, rope // 2)
    frequency = jnp.zeros((1, 128), jnp.float32)
    for i in range(rope // 2):
        frequency = jnp.where(pair == i, rope_base ** (-2.0 * i / rope), frequency)
    low = lax.rem(lane, rope) < rope // 2

    def tables(places):
        angles = places.astype(jnp.float32) * frequency
        sine = jnp.sin(angles)
        return jnp.cos(angles), jnp.where(low, -sine, sine)

    def rotate(values, cosine, sine):
        swapped = jnp.where(
            low, pltpu.roll(values, 128 - rope // 2, 1), pltpu.roll(values, rope // 2, 1)
        )
        return values * cosine + swapped * sine

    def place_of(row):
        return span_ref[row // span_len] * span_len + lax.rem(row, span_len)

    loads[0].wait()
    loads[1].wait()
    own_row = ctx * T + tp * R
    own_places = place_of(own_row) + lax.broadcasted_iota(jnp.int32, (R, 1), 0)
    part = own_ref[:, latent:].astype(jnp.float32)
    turned = rotate(jnp.concatenate([part, part], axis=1), *tables(own_places)).astype(jnp.bfloat16)

    def block(zz, xx, yy, cc):
        return (((zz * X + xx) * Y + yy) * C + cc) * R

    def rows_at(start, size):
        return keys.at[pl.ds(pl.multiple_of(start, R), size)]

    mine = pl.ds(pl.multiple_of(own_row, R), R)
    keys[mine, :latent] = own_ref[:, :latent]
    keys[mine, latent:] = turned

    token = lax.broadcasted_iota(jnp.int32, (T, 1), 0)
    query_places = jnp.zeros((T, 1), jnp.int32)
    for n in range(T // span_len):
        query_places = jnp.where(
            token // span_len == n, place_of(ctx * T + n * span_len) + lax.rem(token, span_len), query_places
        )
    cosine, sine = tables(query_places)
    first = lane < rope
    loads[2].wait()

    def turn(n, carry):
        values = qr[:, pl.ds(pl.multiple_of(n * 128, 128), 128)].astype(jnp.float32)
        value = rotate(values, cosine, sine) * scale
        row = pl.multiple_of(2 * n * T, T)
        queries[pl.ds(row, T), latent:] = jnp.where(first, value, 0.0).astype(jnp.bfloat16)
        queries[pl.ds(row + T, T), latent:] = jnp.where(first, 0.0, value).astype(jnp.bfloat16)
        return carry

    lax.fori_loop(0, H // 2, turn, 0)
    key_lane = lax.broadcasted_iota(jnp.int32, (1, L), 1)
    for n, plane in enumerate(planes):
        key_places = jnp.zeros((1, L), jnp.int32)
        for b in range(L // span_len):
            start = plane * L + b * span_len
            key_places = jnp.where(key_lane // span_len == b, place_of(start) + lax.rem(key_lane, span_len), key_places)
        bias[n] = jnp.where(key_places <= query_places, 0.0, fill_score)
    loads[3].wait()
    loads[4].wait()

    def absorb(n, carry):
        value = jnp.dot(
            qp[:, pl.ds(pl.multiple_of(n * plain, plain), plain)], ku[n], preferred_element_type=jnp.float32
        )
        queries[pl.ds(pl.multiple_of(n * T, T), T), :latent] = (value * scale).astype(jnp.bfloat16)
        return carry

    lax.fori_loop(0, H, absorb, 0, unroll=4)

    pl.semaphore_wait(barrier, len(peers))
    sends = []

    def send(ref, send_sem, recv_sem, device):
        copy = pltpu.make_async_remote_copy(ref, ref, send_sem, recv_sem, device, MESH)
        copy.start()
        sends.append(copy)

    def arrival(ref, send_sem, recv_sem, device):
        pltpu.make_async_remote_copy(ref, ref, send_sem, recv_sem, device, MESH).wait_recv()

    def send_sibling(n, kind):
        ref = rows_at(block(planes[n], *plane_cols(kind), c), R)
        send(ref, ss.at[n, kind], sr.at[n, kind], sibling)

    def send_plane(n):
        ref = rows_at(block(planes[n], x, y, c), R)
        for kind in (2, 0, 1):
            send(ref, ps.at[kind, n], pr.at[kind, planes[n]], plane_devs[kind])
        send_sibling(n, 0)

    def relay_plane(n):
        zz = planes[n]
        arrival(rows_at(block(zz, x, y, c), R), zs.at[n - 1], zr.at[zz], z_dev(zz))
        send_plane(n)

    def relay_sibling(n):
        for kind in (0, 1, 2):
            ref = rows_at(block(planes[n], *plane_cols(kind + 1), c), R)
            arrival(ref, ps.at[kind, n], pr.at[kind, planes[n]], plane_devs[kind])
            send_sibling(n, kind + 1)

    def await_sibling(n):
        for kind in range(4):
            ref = rows_at(block(planes[n], *plane_cols(kind), C - 1 - c), R)
            arrival(ref, ss.at[n, kind], sr.at[n, kind], sibling)

    group = 8

    def plane_rows(n):
        return pl.ds(pl.multiple_of(planes[n] * L, L), L)

    def score(n):
        def step(m, carry):
            start = pl.multiple_of(m * (group * T), group * T)
            value = lax.dot_general(
                queries[pl.ds(start, group * T), :], keys[plane_rows(n), :],
                (((1,), (1,)), ((), ())), preferred_element_type=jnp.float32,
            )
            for g in range(group):
                scores[n, pl.ds(start + g * T, T), :] = value[g * T:(g + 1) * T] + bias[n]
            return carry

        lax.fori_loop(0, H // group, step, 0)

    def attend(members, opening, closing):
        def step(h, carry):
            rows = pl.ds(pl.multiple_of(h * T, T), T)
            tiles = [scores[n, rows, k:k + 128] for n in members for k in range(0, L, 128)]
            highest = tiles[0]
            for tile in tiles[1:]:
                highest = jnp.maximum(highest, tile)
            highest = jnp.max(highest, axis=1, keepdims=True)
            if not opening:
                before = top[rows, :1]
                highest = jnp.maximum(highest, before)
                factor = jnp.exp2(before - highest)
            weights = []
            sums = None
            for tile in tiles:
                raised = jnp.exp2(tile - highest)
                sums = raised if sums is None else sums + raised
                weights.append(raised.astype(jnp.bfloat16))
            summed = None
            per = L // 128
            for i, n in enumerate(members):
                value = jnp.dot(
                    jnp.concatenate(weights[i * per:(i + 1) * per], axis=1), keys[plane_rows(n), :latent],
                    preferred_element_type=jnp.float32,
                )
                summed = value if summed is None else summed + value
            if not opening:
                sums = sums + total[rows, :] * factor
                summed = summed + acc[rows, :] * factor
            if closing:
                context = (summed * (1.0 / jnp.sum(sums, axis=1, keepdims=True))).astype(jnp.bfloat16)
                value = jnp.dot(context, vu[h], preferred_element_type=jnp.float32).astype(jnp.bfloat16)
                width = vu.shape[2]
                heads_out[:, pl.ds(pl.multiple_of(h * width, width), width)] = value
            else:
                top[rows, :] = jnp.broadcast_to(highest, (T, 128))
                total[rows, :] = sums
                acc[rows, :] = summed
            return carry

        lax.fori_loop(0, H, step, 0, unroll=4)

    for n in range(1, Z):
        send(rows_at(own_row, R), zs.at[n - 1], zr.at[z], z_dev(planes[n]))
    send_plane(0)

    relay_sibling(0)
    for n in range(1, Z - 1):
        relay_plane(n)
    await_sibling(0)
    score(0)
    relay_plane(Z - 1)
    relay_sibling(1)
    attend([0], True, False)
    for n in range(1, Z):
        if n + 1 < Z:
            relay_sibling(n + 1)
        await_sibling(n)
        score(n)
        if n == 1:
            attend([1], False, False)
    loads[5].wait()
    attend(list(range(2, Z)), False, True)
    loads[6].wait()

    def project(owner):
        return jnp.dot(
            heads_out[...], w[:, pl.ds(pl.multiple_of(owner * cols, 128), cols)],
            preferred_element_type=jnp.float32,
        )

    for j in (1, 0):
        target = lax.rem(y + j, Y) * C
        sib_out[j] = project(target + C - 1 - c).astype(jnp.bfloat16)
        copy = pltpu.make_async_remote_copy(sib_out.at[j], sib_in.at[j], rss.at[j], rsr.at[j], sibling, MESH)
        copy.start()
        own_part[...] = project(target + c)
        copy.wait_recv()
        sends.append(copy)
        if j > 0:
            y_out[...] = (own_part[...] + sib_in[j].astype(jnp.float32)).astype(jnp.bfloat16)
            y_copy = pltpu.make_async_remote_copy(y_out, y_in, rys.at[0], ryr.at[0], y_peer, MESH)
            y_copy.start()
            sends.append(y_copy)
    result = own_part[...] + sib_in[0].astype(jnp.float32)
    y_copy.wait_recv()
    out_ref[...] = (result + y_in[...].astype(jnp.float32)).astype(out_ref.dtype)
    for copy in sends:
        copy.wait_send()


def fused(dims, *arrays):
    Z, X, Y, C = dims
    query_plain, query_rotary, latent_keys, span_order, key_up, value_up, output_weight = arrays
    T = query_plain.shape[0]
    R = latent_keys.shape[0]
    H, plain, latent = key_up.shape
    tokens = R * Z * X * Y * C
    L = X * Y * C * R
    span_len = tokens // span_order.shape[0]
    cols = output_weight.shape[1] // (Y * C)
    bf16, f32 = jnp.bfloat16, jnp.float32
    dma = pltpu.SemaphoreType.DMA
    operands = (span_order, latent_keys, query_plain, query_rotary, key_up, value_up, output_weight)
    return pl.pallas_call(
        partial(fused_kernel, dims, span_len, latent),
        out_shape=pltpu.VMEM((T, cols), bf16),
        in_specs=[pl.BlockSpec(memory_space=pltpu.HBM)] * len(operands),
        out_specs=pl.BlockSpec(memory_space=pltpu.VMEM),
        scratch_shapes=[
            pltpu.SMEM(span_order.shape, jnp.int32),
            pltpu.VMEM(latent_keys.shape, bf16),
            pltpu.VMEM(query_plain.shape, bf16),
            pltpu.VMEM(query_rotary.shape, bf16),
            pltpu.VMEM(key_up.shape, bf16),
            pltpu.VMEM(value_up.shape, bf16),
            pltpu.VMEM(output_weight.shape, bf16),
            pltpu.VMEM((tokens, latent + 128), bf16),
            pltpu.VMEM((H * T, latent + 128), bf16),
            pltpu.VMEM((Z, T, L), f32),
            pltpu.VMEM((Z, H * T, L), f32),
            pltpu.VMEM((H * T, latent), f32),
            pltpu.VMEM((H * T, 128), f32),
            pltpu.VMEM((H * T, 128), f32),
            pltpu.VMEM((T, H * value_up.shape[2]), bf16),
            pltpu.VMEM((T, cols), f32),
            pltpu.VMEM((Y, T, cols), bf16),
            pltpu.VMEM((Y, T, cols), bf16),
            pltpu.VMEM((T, cols), bf16),
            pltpu.VMEM((T, cols), bf16),
            dma((7,)),
            dma((Z - 1,)), dma((Z,)),
            dma((3, Z)), dma((3, Z)),
            dma((Z, 4)), dma((Z, 4)),
            dma((Y,)), dma((Y,)),
            dma((1,)), dma((1,)),
        ],
        compiler_params=pltpu.CompilerParams(
            collective_id=0, has_side_effects=True, vmem_limit_bytes=56 * 1024 * 1024
        ),
    )(*(pltpu.with_memory_space_constraint(value, pltpu.HBM) for value in operands))


def chosen(mesh, *arrays):
    dims = split_axes(mesh)
    Z, X, Y, C = dims
    query_plain, query_rotary, latent_keys, span_order, key_up, value_up, output_weight = arrays
    R, T = latent_keys.shape[0], query_plain.shape[0]
    rope = latent_keys.shape[1] - key_up.shape[2]
    cols = output_weight.shape[1] // mesh.shape["tp"]
    fits = Z > 1 and X == Y == 2 and mesh.shape["tp"] == 4 and R % 16 == 0 and cols % 128 == 0
    fits = fits and rope * 2 == 128 and (X * Y * C * R) % 128 == 0 and key_up.shape[0] % 8 == 0
    return fused(dims, *arrays) if fits else on_device(*arrays)


def solution(mesh):
    return jax.shard_map(
        partial(chosen, mesh),
        mesh=mesh,
        in_specs=(
            P("ctx", "tp"),
            P("ctx", "tp"),
            P(("ctx", "tp"), None),
            P(),
            P("tp", None, None),
            P("tp", None, None),
            P("tp", None),
        ),
        out_specs=P("ctx", "tp"),
        check_vma=False,
    )
```

```python
import math
from functools import partial

import jax
import jax.numpy as jnp
from jax import lax
from jax.experimental import pallas as pl
from jax.experimental.pallas import tpu as pltpu
from jax.sharding import PartitionSpec as P

rope_base = 10000.0
fill_score = -1e30
key_block_rows = 512


def rotate_pairs(values, places):
    halfway = values.shape[-1] // 2
    frequency = rope_base ** (-jnp.arange(halfway, dtype=jnp.float32) * 2.0 / values.shape[-1])
    angles = places.astype(jnp.float32)[:, None] * frequency[None, :]
    cosine = jnp.cos(angles)
    sine_part = jnp.sin(angles)
    if values.ndim == 3:
        cosine = cosine[:, None, :]
        sine_part = sine_part[:, None, :]
    first_half = values[..., :halfway]
    second_half = values[..., halfway:]
    return jnp.concatenate(
        [
            first_half * cosine - second_half * sine_part,
            first_half * sine_part + second_half * cosine,
        ],
        axis=-1,
    )


def token_places(span_table, indices, span_len):
    slot_ids = indices // span_len
    slot_table = jnp.arange(span_table.shape[0], dtype=jnp.int32)
    picked = jnp.sum(
        jnp.where(slot_ids[:, None] == slot_table[None, :], span_table[None, :], 0), axis=1
    )
    return picked * span_len + indices % span_len


def attend_block(
    carry_state, keys_block, key_places, queries, query_places, latent_width, score_scale
):
    running_max, running_sum, summed = carry_state
    scores = jnp.dot(queries, keys_block.T, preferred_element_type=jnp.float32) * score_scale
    allowed = key_places[None, :] <= query_places[:, None]
    masked = jnp.where(allowed, scores, fill_score)
    new_max = jnp.maximum(running_max, jnp.max(masked, axis=1))
    weights = jnp.where(allowed, jnp.exp(scores - new_max[:, None]), 0.0)
    factor = jnp.exp(running_max - new_max)
    new_sum = running_sum * factor + jnp.sum(weights, axis=1)
    new_summed = summed * factor[:, None] + jnp.dot(
        weights.astype(jnp.bfloat16),
        keys_block[:, :latent_width],
        preferred_element_type=jnp.float32,
    )
    return (new_max, new_sum, new_summed)


def attend_guarded(
    carry_state, keys_block, key_places, queries, query_places, latest, latent_width, score_scale
):
    return lax.cond(
        jnp.min(key_places) > latest,
        lambda carried: carried,
        lambda carried: attend_block(
            carried, keys_block, key_places, queries, query_places, latent_width, score_scale
        ),
        carry_state,
    )


def make_folder(queries, row_places, latest, span_order, span_len, latent_width, score_scale):

    def fold_piece(carry_state, key_piece, offset):
        piece_rows = key_piece.shape[0]
        key_places = token_places(span_order, jnp.arange(piece_rows, dtype=jnp.int32), span_len)

        def step_block(carried, block_parts):
            return (
                attend_guarded(
                    carried,
                    block_parts[0],
                    block_parts[1],
                    queries,
                    row_places,
                    latest,
                    latent_width,
                    score_scale,
                ),
                None,
            )

        stacked = key_piece.reshape(
            piece_rows // key_block_rows, key_block_rows, key_piece.shape[1]
        )
        stacked_places = key_places.reshape(piece_rows // key_block_rows, key_block_rows)
        result_state, unused = lax.scan(step_block, carry_state, (stacked, stacked_places))
        return result_state

    return fold_piece


def start_state(row_count, latent_width):
    return (
        jnp.full((row_count,), fill_score, jnp.float32),
        jnp.zeros((row_count,), jnp.float32),
        jnp.zeros((row_count,), jnp.float32)[:, None] + jnp.zeros((1, latent_width), jnp.float32),
    )


def project_out(final_state, token_count, head_count, latent_width, value_up, output_weight):
    running_max, running_sum, summed = final_state
    mixed_latent = (
        (summed / running_sum[:, None])
        .astype(jnp.bfloat16)
        .reshape(token_count, head_count, latent_width)
    )
    head_out = jnp.einsum(
        "thl,hlv->thv", mixed_latent, value_up, preferred_element_type=jnp.float32
    ).astype(jnp.bfloat16)
    head_out = head_out.reshape(token_count, head_count * value_up.shape[2])
    return jnp.dot(head_out, output_weight, preferred_element_type=jnp.float32)


def on_device(query_plain, query_rotary, latent_keys, span_order, key_up, value_up, output_weight):
    local_tokens = query_plain.shape[0]
    head_count = key_up.shape[0]
    plain_width = key_up.shape[1]
    latent_width = key_up.shape[2]
    rotary_width = query_rotary.shape[1] // head_count
    span_len = local_tokens // 2
    score_scale = 1.0 / math.sqrt(plain_width + rotary_width)
    first_row = lax.axis_index("ctx") * local_tokens
    query_places = token_places(
        span_order, first_row + jnp.arange(local_tokens, dtype=jnp.int32), span_len
    )
    absorbed = jnp.einsum(
        "thn,hnl->thl",
        query_plain.reshape(local_tokens, head_count, plain_width),
        key_up,
        preferred_element_type=jnp.float32,
    ).astype(jnp.bfloat16)
    turned = rotate_pairs(
        query_rotary.reshape(local_tokens, head_count, rotary_width).astype(jnp.float32),
        query_places,
    ).astype(jnp.bfloat16)
    queries = jnp.concatenate([absorbed, turned], axis=2).reshape(
        local_tokens * head_count, latent_width + rotary_width
    )
    row_places = jnp.repeat(query_places, head_count)
    own_rows = latent_keys.shape[0]
    own_first = first_row + lax.axis_index("tp") * own_rows
    own_places = token_places(
        span_order, own_first + jnp.arange(own_rows, dtype=jnp.int32), span_len
    )
    own_turned = rotate_pairs(latent_keys[:, latent_width:].astype(jnp.float32), own_places).astype(
        jnp.bfloat16
    )
    own_keys = jnp.concatenate([latent_keys[:, :latent_width], own_turned], axis=1)
    latest = jnp.max(query_places)
    folder = make_folder(
        queries, row_places, latest, span_order, span_len, latent_width, score_scale
    )
    group_keys = lax.all_gather(own_keys, "tp", axis=0, tiled=True)
    final_state = folder(
        start_state(local_tokens * head_count, latent_width),
        lax.all_gather(group_keys, "ctx", axis=0, tiled=True),
        jnp.int32(0),
    )
    head_terms = project_out(
        final_state, local_tokens, head_count, latent_width, value_up, output_weight
    )
    return lax.psum_scatter(head_terms.astype(jnp.bfloat16), "tp", scatter_dimension=1, tiled=True)


MESH = pl.DeviceIdType.MESH


def split_axes(mesh):
    ctx, tp = mesh.shape["ctx"], mesh.shape["tp"]
    x_size = 1
    while (2 * x_size) ** 2 <= ctx and ctx % (2 * x_size) == 0:
        x_size *= 2
    return ctx // x_size, x_size, tp // 2, 2


def fused_kernel(dims, span_len, latent, span_hbm, own_hbm, qp_hbm, qr_hbm, ku_hbm, vu_hbm, w_hbm,
                 out_ref, span_ref, own_ref, qp, qr, ku, vu, w, keys, queries, bias, scores, acc, top, total,
                 heads_out, own_part, sib_out, sib_in, y_out, y_in,
                 load_sem, zs, zr, ps, pr, ss, sr, rss, rsr, rys, ryr):
    Z, X, Y, C = dims
    ctx = lax.axis_index("ctx")
    tp = lax.axis_index("tp")
    z, x = ctx // X, ctx % X
    y, c = tp // C, tp % C
    R = own_ref.shape[0]
    rope = own_ref.shape[1] - latent
    T = qp.shape[0]
    H, plain = ku.shape[0], ku.shape[1]
    L = X * Y * C * R
    cols = out_ref.shape[1]
    scale = math.log2(math.e) / math.sqrt(plain + rope)

    def z_dev(zz):
        return (zz * X + x, tp)

    sibling = (ctx, y * C + (C - 1 - c))
    y_peer = (ctx, (1 - y) * C + c)
    plane_devs = [(z * X + 1 - x, tp), y_peer, (z * X + 1 - x, (1 - y) * C + c)]

    def plane_cols(kind):
        return [(x, y), (1 - x, y), (x, 1 - y), (1 - x, 1 - y)][kind]

    def z_order(i):
        low = i + (i >= z).astype(jnp.int32)
        high = Z - 1 - i - (i >= Z - 1 - z).astype(jnp.int32)
        return jnp.where(z < Z // 2, low, high)

    planes = [z] + [z_order(jnp.int32(i)) for i in range(Z - 1)]

    barrier = pltpu.get_barrier_semaphore()
    peers = [z_dev(zz) for zz in planes[1:]] + plane_devs + [sibling]
    for peer in peers:
        pl.semaphore_signal(barrier, inc=1, device_id=peer, device_id_type=MESH)

    loads = []
    pairs = ((own_hbm, own_ref), (span_hbm, span_ref), (qr_hbm, qr), (qp_hbm, qp), (ku_hbm, ku), (vu_hbm, vu), (w_hbm, w))
    for n, (src, dst) in enumerate(pairs):
        load = pltpu.make_async_copy(src, dst, load_sem.at[n])
        load.start()
        loads.append(load)

    lane = lax.broadcasted_iota(jnp.int32, (1, 128), 1)
    pair = lax.rem(lane, rope // 2)
    frequency = jnp.zeros((1, 128), jnp.float32)
    for i in range(rope // 2):
        frequency = jnp.where(pair == i, rope_base ** (-2.0 * i / rope), frequency)
    low = lax.rem(lane, rope) < rope // 2

    def tables(places):
        angles = places.astype(jnp.float32) * frequency
        sine = jnp.sin(angles)
        return jnp.cos(angles), jnp.where(low, -sine, sine)

    def rotate(values, cosine, sine):
        swapped = jnp.where(
            low, pltpu.roll(values, 128 - rope // 2, 1), pltpu.roll(values, rope // 2, 1)
        )
        return values * cosine + swapped * sine

    def place_of(row):
        return span_ref[row // span_len] * span_len + lax.rem(row, span_len)

    loads[0].wait()
    loads[1].wait()
    own_row = ctx * T + tp * R
    own_places = place_of(own_row) + lax.broadcasted_iota(jnp.int32, (R, 1), 0)
    part = own_ref[:, latent:].astype(jnp.float32)
    turned = rotate(jnp.concatenate([part, part], axis=1), *tables(own_places)).astype(jnp.bfloat16)

    def block(zz, xx, yy, cc):
        return (((zz * X + xx) * Y + yy) * C + cc) * R

    def rows_at(start, size):
        return keys.at[pl.ds(pl.multiple_of(start, R), size)]

    mine = pl.ds(pl.multiple_of(own_row, R), R)
    keys[mine, :latent] = own_ref[:, :latent]
    keys[mine, latent:] = turned

    token = lax.broadcasted_iota(jnp.int32, (T, 1), 0)
    query_places = jnp.zeros((T, 1), jnp.int32)
    for n in range(T // span_len):
        query_places = jnp.where(
            token // span_len == n, place_of(ctx * T + n * span_len) + lax.rem(token, span_len), query_places
        )
    cosine, sine = tables(query_places)
    first = lane < rope
    loads[2].wait()

    def turn(n, carry):
        values = qr[:, pl.ds(pl.multiple_of(n * 128, 128), 128)].astype(jnp.float32)
        value = rotate(values, cosine, sine) * scale
        row = pl.multiple_of(2 * n * T, T)
        queries[pl.ds(row, T), latent:] = jnp.where(first, value, 0.0).astype(jnp.bfloat16)
        queries[pl.ds(row + T, T), latent:] = jnp.where(first, 0.0, value).astype(jnp.bfloat16)
        return carry

    lax.fori_loop(0, H // 2, turn, 0)
    key_lane = lax.broadcasted_iota(jnp.int32, (1, L), 1)
    for n, plane in enumerate(planes):
        key_places = jnp.zeros((1, L), jnp.int32)
        for b in range(L // span_len):
            start = plane * L + b * span_len
            key_places = jnp.where(key_lane // span_len == b, place_of(start) + lax.rem(key_lane, span_len), key_places)
        bias[n] = jnp.where(key_places <= query_places, 0.0, fill_score)
    loads[3].wait()
    loads[4].wait()

    def absorb(n, carry):
        value = jnp.dot(
            qp[:, pl.ds(pl.multiple_of(n * plain, plain), plain)], ku[n], preferred_element_type=jnp.float32
        )
        queries[pl.ds(pl.multiple_of(n * T, T), T), :latent] = (value * scale).astype(jnp.bfloat16)
        return carry

    lax.fori_loop(0, H, absorb, 0, unroll=4)

    pl.semaphore_wait(barrier, len(peers))
    sends = []

    def send(ref, send_sem, recv_sem, device):
        copy = pltpu.make_async_remote_copy(ref, ref, send_sem, recv_sem, device, MESH)
        copy.start()
        sends.append(copy)

    def arrival(ref, send_sem, recv_sem, device):
        pltpu.make_async_remote_copy(ref, ref, send_sem, recv_sem, device, MESH).wait_recv()

    def send_sibling(n, kind):
        ref = rows_at(block(planes[n], *plane_cols(kind), c), R)
        send(ref, ss.at[n, kind], sr.at[n, kind], sibling)

    def send_plane(n):
        ref = rows_at(block(planes[n], x, y, c), R)
        for kind in (2, 0, 1):
            send(ref, ps.at[kind, n], pr.at[kind, planes[n]], plane_devs[kind])
        send_sibling(n, 0)

    def relay_plane(n):
        zz = planes[n]
        arrival(rows_at(block(zz, x, y, c), R), zs.at[n - 1], zr.at[zz], z_dev(zz))
        send_plane(n)

    def relay_sibling(n):
        for kind in (0, 1, 2):
            ref = rows_at(block(planes[n], *plane_cols(kind + 1), c), R)
            arrival(ref, ps.at[kind, n], pr.at[kind, planes[n]], plane_devs[kind])
            send_sibling(n, kind + 1)

    def await_sibling(n):
        for kind in range(4):
            ref = rows_at(block(planes[n], *plane_cols(kind), C - 1 - c), R)
            arrival(ref, ss.at[n, kind], sr.at[n, kind], sibling)

    group = 8

    def plane_rows(n):
        return pl.ds(pl.multiple_of(planes[n] * L, L), L)

    def score(n):
        def step(m, carry):
            start = pl.multiple_of(m * (group * T), group * T)
            value = lax.dot_general(
                queries[pl.ds(start, group * T), :], keys[plane_rows(n), :],
                (((1,), (1,)), ((), ())), preferred_element_type=jnp.float32,
            )
            for g in range(group):
                scores[n, pl.ds(start + g * T, T), :] = value[g * T:(g + 1) * T] + bias[n]
            return carry

        lax.fori_loop(0, H // group, step, 0)

    def attend(members, opening, closing, begin=0, end=H):
        def step(h, carry):
            rows = pl.ds(pl.multiple_of(h * T, T), T)
            tiles = [scores[n, rows, k:k + 128] for n in members for k in range(0, L, 128)]
            highest = tiles[0]
            for tile in tiles[1:]:
                highest = jnp.maximum(highest, tile)
            highest = jnp.max(highest, axis=1, keepdims=True)
            if not opening:
                before = top[rows, :1]
                highest = jnp.maximum(highest, before)
                factor = jnp.exp2(before - highest)
            weights = []
            sums = None
            for tile in tiles:
                raised = jnp.exp2(tile - highest)
                sums = raised if sums is None else sums + raised
                weights.append(raised.astype(jnp.bfloat16))
            summed = None
            per = L // 128
            for i, n in enumerate(members):
                value = jnp.dot(
                    jnp.concatenate(weights[i * per:(i + 1) * per], axis=1), keys[plane_rows(n), :latent],
                    preferred_element_type=jnp.float32,
                )
                summed = value if summed is None else summed + value
            if not opening:
                sums = sums + total[rows, :] * factor
                summed = summed + acc[rows, :] * factor
            if closing:
                context = (summed * (1.0 / jnp.sum(sums, axis=1, keepdims=True))).astype(jnp.bfloat16)
                value = jnp.dot(context, vu[h], preferred_element_type=jnp.float32).astype(jnp.bfloat16)
                width = vu.shape[2]
                heads_out[:, pl.ds(pl.multiple_of(h * width, width), width)] = value
            else:
                top[rows, :] = jnp.broadcast_to(highest, (T, 128))
                total[rows, :] = sums
                acc[rows, :] = summed
            return carry

        lax.fori_loop(begin, end, step, 0, unroll=8)

    for n in range(1, Z):
        send(rows_at(own_row, R), zs.at[n - 1], zr.at[z], z_dev(planes[n]))
    send_plane(0)

    relay_sibling(0)
    for n in range(1, Z):
        relay_plane(n)
    relay_sibling(1)
    half = Z // 2
    for n in range(half):
        await_sibling(n)
        score(n)
    for n in range(half, Z):
        relay_sibling(n)
        part = H // (Z - half)
        attend(list(range(half)), True, False, (n - half) * part, (n - half + 1) * part)
    for n in range(half, Z):
        await_sibling(n)
        score(n)
    loads[5].wait()
    attend(list(range(half, Z)), False, True)
    loads[6].wait()

    def project(owner):
        return jnp.dot(
            heads_out[...], w[:, pl.ds(pl.multiple_of(owner * cols, 128), cols)],
            preferred_element_type=jnp.float32,
        )

    for j in (1, 0):
        target = lax.rem(y + j, Y) * C
        sib_out[j] = project(target + C - 1 - c).astype(jnp.bfloat16)
        copy = pltpu.make_async_remote_copy(sib_out.at[j], sib_in.at[j], rss.at[j], rsr.at[j], sibling, MESH)
        copy.start()
        own_part[...] = project(target + c)
        copy.wait_recv()
        sends.append(copy)
        if j > 0:
            y_out[...] = (own_part[...] + sib_in[j].astype(jnp.float32)).astype(jnp.bfloat16)
            y_copy = pltpu.make_async_remote_copy(y_out, y_in, rys.at[0], ryr.at[0], y_peer, MESH)
            y_copy.start()
            sends.append(y_copy)
    result = own_part[...] + sib_in[0].astype(jnp.float32)
    y_copy.wait_recv()
    out_ref[...] = (result + y_in[...].astype(jnp.float32)).astype(out_ref.dtype)
    for copy in sends:
        copy.wait_send()


def fused(dims, *arrays):
    Z, X, Y, C = dims
    query_plain, query_rotary, latent_keys, span_order, key_up, value_up, output_weight = arrays
    T = query_plain.shape[0]
    R = latent_keys.shape[0]
    H, plain, latent = key_up.shape
    tokens = R * Z * X * Y * C
    L = X * Y * C * R
    span_len = tokens // span_order.shape[0]
    cols = output_weight.shape[1] // (Y * C)
    bf16, f32 = jnp.bfloat16, jnp.float32
    dma = pltpu.SemaphoreType.DMA
    operands = (span_order, latent_keys, query_plain, query_rotary, key_up, value_up, output_weight)
    return pl.pallas_call(
        partial(fused_kernel, dims, span_len, latent),
        out_shape=pltpu.VMEM((T, cols), bf16),
        in_specs=[pl.BlockSpec(memory_space=pltpu.HBM)] * len(operands),
        out_specs=pl.BlockSpec(memory_space=pltpu.VMEM),
        scratch_shapes=[
            pltpu.SMEM(span_order.shape, jnp.int32),
            pltpu.VMEM(latent_keys.shape, bf16),
            pltpu.VMEM(query_plain.shape, bf16),
            pltpu.VMEM(query_rotary.shape, bf16),
            pltpu.VMEM(key_up.shape, bf16),
            pltpu.VMEM(value_up.shape, bf16),
            pltpu.VMEM(output_weight.shape, bf16),
            pltpu.VMEM((tokens, latent + 128), bf16),
            pltpu.VMEM((H * T, latent + 128), bf16),
            pltpu.VMEM((Z, T, L), f32),
            pltpu.VMEM((Z, H * T, L), f32),
            pltpu.VMEM((H * T, latent), f32),
            pltpu.VMEM((H * T, 128), f32),
            pltpu.VMEM((H * T, 128), f32),
            pltpu.VMEM((T, H * value_up.shape[2]), bf16),
            pltpu.VMEM((T, cols), f32),
            pltpu.VMEM((Y, T, cols), bf16),
            pltpu.VMEM((Y, T, cols), bf16),
            pltpu.VMEM((T, cols), bf16),
            pltpu.VMEM((T, cols), bf16),
            dma((7,)),
            dma((Z - 1,)), dma((Z,)),
            dma((3, Z)), dma((3, Z)),
            dma((Z, 4)), dma((Z, 4)),
            dma((Y,)), dma((Y,)),
            dma((1,)), dma((1,)),
        ],
        compiler_params=pltpu.CompilerParams(
            collective_id=0, has_side_effects=True, vmem_limit_bytes=56 * 1024 * 1024
        ),
    )(*(pltpu.with_memory_space_constraint(value, pltpu.HBM) for value in operands))


def chosen(mesh, *arrays):
    dims = split_axes(mesh)
    Z, X, Y, C = dims
    query_plain, query_rotary, latent_keys, span_order, key_up, value_up, output_weight = arrays
    R, T = latent_keys.shape[0], query_plain.shape[0]
    rope = latent_keys.shape[1] - key_up.shape[2]
    cols = output_weight.shape[1] // mesh.shape["tp"]
    fits = Z > 1 and X == Y == 2 and mesh.shape["tp"] == 4 and R % 16 == 0 and cols % 128 == 0
    fits = fits and rope * 2 == 128 and (X * Y * C * R) % 128 == 0 and key_up.shape[0] % 8 == 0 and key_up.shape[0] % (Z - Z // 2) == 0
    return fused(dims, *arrays) if fits else on_device(*arrays)


def solution(mesh):
    return jax.shard_map(
        partial(chosen, mesh),
        mesh=mesh,
        in_specs=(
            P("ctx", "tp"),
            P("ctx", "tp"),
            P(("ctx", "tp"), None),
            P(),
            P("tp", None, None),
            P("tp", None, None),
            P("tp", None),
        ),
        out_specs=P("ctx", "tp"),
        check_vma=False,
    )
```

```python
import math
from functools import partial

import jax
import jax.numpy as jnp
from jax import lax
from jax.experimental import pallas as pl
from jax.experimental.pallas import tpu as pltpu
from jax.sharding import PartitionSpec as P

rope_base = 10000.0
fill_score = -1e30
key_block_rows = 512


def rotate_pairs(values, places):
    halfway = values.shape[-1] // 2
    frequency = rope_base ** (-jnp.arange(halfway, dtype=jnp.float32) * 2.0 / values.shape[-1])
    angles = places.astype(jnp.float32)[:, None] * frequency[None, :]
    cosine = jnp.cos(angles)
    sine_part = jnp.sin(angles)
    if values.ndim == 3:
        cosine = cosine[:, None, :]
        sine_part = sine_part[:, None, :]
    first_half = values[..., :halfway]
    second_half = values[..., halfway:]
    return jnp.concatenate(
        [
            first_half * cosine - second_half * sine_part,
            first_half * sine_part + second_half * cosine,
        ],
        axis=-1,
    )


def token_places(span_table, indices, span_len):
    slot_ids = indices // span_len
    slot_table = jnp.arange(span_table.shape[0], dtype=jnp.int32)
    picked = jnp.sum(
        jnp.where(slot_ids[:, None] == slot_table[None, :], span_table[None, :], 0), axis=1
    )
    return picked * span_len + indices % span_len


def attend_block(
    carry_state, keys_block, key_places, queries, query_places, latent_width, score_scale
):
    running_max, running_sum, summed = carry_state
    scores = jnp.dot(queries, keys_block.T, preferred_element_type=jnp.float32) * score_scale
    allowed = key_places[None, :] <= query_places[:, None]
    masked = jnp.where(allowed, scores, fill_score)
    new_max = jnp.maximum(running_max, jnp.max(masked, axis=1))
    weights = jnp.where(allowed, jnp.exp(scores - new_max[:, None]), 0.0)
    factor = jnp.exp(running_max - new_max)
    new_sum = running_sum * factor + jnp.sum(weights, axis=1)
    new_summed = summed * factor[:, None] + jnp.dot(
        weights.astype(jnp.bfloat16),
        keys_block[:, :latent_width],
        preferred_element_type=jnp.float32,
    )
    return (new_max, new_sum, new_summed)


def attend_guarded(
    carry_state, keys_block, key_places, queries, query_places, latest, latent_width, score_scale
):
    return lax.cond(
        jnp.min(key_places) > latest,
        lambda carried: carried,
        lambda carried: attend_block(
            carried, keys_block, key_places, queries, query_places, latent_width, score_scale
        ),
        carry_state,
    )


def make_folder(queries, row_places, latest, span_order, span_len, latent_width, score_scale):

    def fold_piece(carry_state, key_piece, offset):
        piece_rows = key_piece.shape[0]
        key_places = token_places(span_order, jnp.arange(piece_rows, dtype=jnp.int32), span_len)

        def step_block(carried, block_parts):
            return (
                attend_guarded(
                    carried,
                    block_parts[0],
                    block_parts[1],
                    queries,
                    row_places,
                    latest,
                    latent_width,
                    score_scale,
                ),
                None,
            )

        stacked = key_piece.reshape(
            piece_rows // key_block_rows, key_block_rows, key_piece.shape[1]
        )
        stacked_places = key_places.reshape(piece_rows // key_block_rows, key_block_rows)
        result_state, unused = lax.scan(step_block, carry_state, (stacked, stacked_places))
        return result_state

    return fold_piece


def start_state(row_count, latent_width):
    return (
        jnp.full((row_count,), fill_score, jnp.float32),
        jnp.zeros((row_count,), jnp.float32),
        jnp.zeros((row_count,), jnp.float32)[:, None] + jnp.zeros((1, latent_width), jnp.float32),
    )


def project_out(final_state, token_count, head_count, latent_width, value_up, output_weight):
    running_max, running_sum, summed = final_state
    mixed_latent = (
        (summed / running_sum[:, None])
        .astype(jnp.bfloat16)
        .reshape(token_count, head_count, latent_width)
    )
    head_out = jnp.einsum(
        "thl,hlv->thv", mixed_latent, value_up, preferred_element_type=jnp.float32
    ).astype(jnp.bfloat16)
    head_out = head_out.reshape(token_count, head_count * value_up.shape[2])
    return jnp.dot(head_out, output_weight, preferred_element_type=jnp.float32)


def on_device(query_plain, query_rotary, latent_keys, span_order, key_up, value_up, output_weight):
    local_tokens = query_plain.shape[0]
    head_count = key_up.shape[0]
    plain_width = key_up.shape[1]
    latent_width = key_up.shape[2]
    rotary_width = query_rotary.shape[1] // head_count
    span_len = local_tokens // 2
    score_scale = 1.0 / math.sqrt(plain_width + rotary_width)
    first_row = lax.axis_index("ctx") * local_tokens
    query_places = token_places(
        span_order, first_row + jnp.arange(local_tokens, dtype=jnp.int32), span_len
    )
    absorbed = jnp.einsum(
        "thn,hnl->thl",
        query_plain.reshape(local_tokens, head_count, plain_width),
        key_up,
        preferred_element_type=jnp.float32,
    ).astype(jnp.bfloat16)
    turned = rotate_pairs(
        query_rotary.reshape(local_tokens, head_count, rotary_width).astype(jnp.float32),
        query_places,
    ).astype(jnp.bfloat16)
    queries = jnp.concatenate([absorbed, turned], axis=2).reshape(
        local_tokens * head_count, latent_width + rotary_width
    )
    row_places = jnp.repeat(query_places, head_count)
    own_rows = latent_keys.shape[0]
    own_first = first_row + lax.axis_index("tp") * own_rows
    own_places = token_places(
        span_order, own_first + jnp.arange(own_rows, dtype=jnp.int32), span_len
    )
    own_turned = rotate_pairs(latent_keys[:, latent_width:].astype(jnp.float32), own_places).astype(
        jnp.bfloat16
    )
    own_keys = jnp.concatenate([latent_keys[:, :latent_width], own_turned], axis=1)
    latest = jnp.max(query_places)
    folder = make_folder(
        queries, row_places, latest, span_order, span_len, latent_width, score_scale
    )
    group_keys = lax.all_gather(own_keys, "tp", axis=0, tiled=True)
    final_state = folder(
        start_state(local_tokens * head_count, latent_width),
        lax.all_gather(group_keys, "ctx", axis=0, tiled=True),
        jnp.int32(0),
    )
    head_terms = project_out(
        final_state, local_tokens, head_count, latent_width, value_up, output_weight
    )
    return lax.psum_scatter(head_terms.astype(jnp.bfloat16), "tp", scatter_dimension=1, tiled=True)


MESH = pl.DeviceIdType.MESH


def split_axes(mesh):
    ctx, tp = mesh.shape["ctx"], mesh.shape["tp"]
    x_size = 1
    while (2 * x_size) ** 2 <= ctx and ctx % (2 * x_size) == 0:
        x_size *= 2
    return ctx // x_size, x_size, tp // 2, 2


def fused_kernel(dims, span_len, latent, span_hbm, own_hbm, qp_hbm, qr_hbm, ku_hbm, vu_hbm, w_hbm,
                 out_ref, span_ref, own_ref, qp, qr, ku, vu, w, keys, queries, bias, scores, acc, top, total,
                 heads_out, own_part, sib_out, sib_in, y_out, y_in,
                 load_sem, plane_sem, line_sem, zs, zr, ps, pr, ss, sr, rss, rsr, rys, ryr):
    Z, X, Y, C = dims
    ctx = lax.axis_index("ctx")
    tp = lax.axis_index("tp")
    z, x = ctx // X, ctx % X
    y, c = tp // C, tp % C
    R = own_ref.shape[0]
    rope = own_ref.shape[1] - latent
    T = qp.shape[0]
    H, plain = ku.shape[0], ku.shape[1]
    L = X * Y * C * R
    cols = out_ref.shape[1]
    scale = math.log2(math.e) / math.sqrt(plain + rope)

    def z_dev(zz):
        return (zz * X + x, tp)

    sibling = (ctx, y * C + (C - 1 - c))
    y_peer = (ctx, (1 - y) * C + c)
    plane_devs = [(z * X + 1 - x, tp), y_peer, (z * X + 1 - x, (1 - y) * C + c)]

    def plane_cols(kind):
        return [(x, y), (1 - x, y), (x, 1 - y), (1 - x, 1 - y)][kind]

    def z_order(i):
        low = i + (i >= z).astype(jnp.int32)
        high = Z - 1 - i - (i >= Z - 1 - z).astype(jnp.int32)
        return jnp.where(z < Z // 2, low, high)

    planes = [z] + [z_order(jnp.int32(i)) for i in range(Z - 1)]

    barrier = pltpu.get_barrier_semaphore()

    def on_line(zz):
        return (zz >= 0) & (zz < Z)

    def greet(semaphore, device):
        pl.semaphore_signal(semaphore, inc=1, device_id=device, device_id_type=MESH)

    for peer in plane_devs[:2] + [sibling]:
        greet(barrier, peer)
    for d in (-1, 1):
        pl.when(on_line(z + d))(partial(greet, barrier, z_dev(z + d)))

    loads = []
    pairs = ((own_hbm, own_ref), (span_hbm, span_ref), (qr_hbm, qr), (qp_hbm, qp), (ku_hbm, ku), (vu_hbm, vu), (w_hbm, w))
    for n, (src, dst) in enumerate(pairs):
        load = pltpu.make_async_copy(src, dst, load_sem.at[n])
        load.start()
        loads.append(load)

    lane = lax.broadcasted_iota(jnp.int32, (1, 128), 1)
    pair = lax.rem(lane, rope // 2)
    frequency = jnp.zeros((1, 128), jnp.float32)
    for i in range(rope // 2):
        frequency = jnp.where(pair == i, rope_base ** (-2.0 * i / rope), frequency)
    low = lax.rem(lane, rope) < rope // 2

    def tables(places):
        angles = places.astype(jnp.float32) * frequency
        sine = jnp.sin(angles)
        return jnp.cos(angles), jnp.where(low, -sine, sine)

    def rotate(values, cosine, sine):
        swapped = jnp.where(
            low, pltpu.roll(values, 128 - rope // 2, 1), pltpu.roll(values, rope // 2, 1)
        )
        return values * cosine + swapped * sine

    def place_of(row):
        return span_ref[row // span_len] * span_len + lax.rem(row, span_len)

    loads[0].wait()
    loads[1].wait()
    own_row = ctx * T + tp * R
    own_places = place_of(own_row) + lax.broadcasted_iota(jnp.int32, (R, 1), 0)
    part = own_ref[:, latent:].astype(jnp.float32)
    turned = rotate(jnp.concatenate([part, part], axis=1), *tables(own_places)).astype(jnp.bfloat16)

    def block(zz, xx, yy, cc):
        return (((zz * X + xx) * Y + yy) * C + cc) * R

    def rows_at(start, size):
        return keys.at[pl.ds(pl.multiple_of(start, R), size)]

    mine = pl.ds(pl.multiple_of(own_row, R), R)
    keys[mine, :latent] = own_ref[:, :latent]
    keys[mine, latent:] = turned

    ends = on_line(z - 1).astype(jnp.int32) + on_line(z + 1).astype(jnp.int32)
    pl.semaphore_wait(barrier, 3 + ends)
    sends = []

    def send(ref, send_sem, recv_sem, device):
        copy = pltpu.make_async_remote_copy(ref, ref, send_sem, recv_sem, device, MESH)
        copy.start()
        sends.append(copy)

    def arrival(ref, send_sem, recv_sem, device):
        pltpu.make_async_remote_copy(ref, ref, send_sem, recv_sem, device, MESH).wait_recv()

    def send_sibling(n, kind):
        ref = rows_at(block(planes[n], *plane_cols(kind), c), R)
        send(ref, ss.at[n, kind], sr.at[n, kind], sibling)

    def send_plane(n):
        ref = rows_at(block(planes[n], x, y, c), R)
        for kind in (2, 0, 1) if n > 0 else (0, 1):
            send(ref, ps.at[kind, n], pr.at[kind, planes[n]], plane_devs[kind])
        send_sibling(n, 0)

    def relay_plane(n):
        zz = planes[n]
        arrival(rows_at(block(zz, x, y, c), R), zs.at[zz], zr.at[zz], z_dev(zz))
        send_plane(n)

    def relay_sibling(n):
        for kind in (0, 1, 2):
            ref = rows_at(block(planes[n], *plane_cols(kind + 1), c), R)
            arrival(ref, ps.at[kind, n], pr.at[kind, planes[n]], plane_devs[kind])
            send_sibling(n, kind + 1)

    def await_sibling(n):
        for kind in range(4):
            ref = rows_at(block(planes[n], *plane_cols(kind), C - 1 - c), R)
            arrival(ref, ss.at[n, kind], sr.at[n, kind], sibling)

    group = 8

    def plane_rows(n):
        return pl.ds(pl.multiple_of(planes[n] * L, L), L)

    def score(n):
        def step(m, carry):
            start = pl.multiple_of(m * (group * T), group * T)
            value = lax.dot_general(
                queries[pl.ds(start, group * T), :], keys[plane_rows(n), :],
                (((1,), (1,)), ((), ())), preferred_element_type=jnp.float32,
            )
            for g in range(group):
                scores[n, pl.ds(start + g * T, T), :] = value[g * T:(g + 1) * T] + bias[n]
            return carry

        lax.fori_loop(0, H // group, step, 0)

    def attend(members, opening, closing, begin=0, end=H):
        def step(h, carry):
            rows = pl.ds(pl.multiple_of(h * T, T), T)
            tiles = [scores[n, rows, k:k + 128] for n in members for k in range(0, L, 128)]
            highest = tiles[0]
            for tile in tiles[1:]:
                highest = jnp.maximum(highest, tile)
            highest = jnp.max(highest, axis=1, keepdims=True)
            if not opening:
                before = top[rows, :1]
                highest = jnp.maximum(highest, before)
                factor = jnp.exp2(before - highest)
            weights = []
            sums = None
            for tile in tiles:
                raised = jnp.exp2(tile - highest)
                sums = raised if sums is None else sums + raised
                weights.append(raised.astype(jnp.bfloat16))
            summed = None
            per = L // 128
            for i, n in enumerate(members):
                value = jnp.dot(
                    jnp.concatenate(weights[i * per:(i + 1) * per], axis=1), keys[plane_rows(n), :latent],
                    preferred_element_type=jnp.float32,
                )
                summed = value if summed is None else summed + value
            if not opening:
                sums = sums + total[rows, :] * factor
                summed = summed + acc[rows, :] * factor
            if closing:
                context = (summed * (1.0 / jnp.sum(sums, axis=1, keepdims=True))).astype(jnp.bfloat16)
                value = jnp.dot(context, vu[h], preferred_element_type=jnp.float32).astype(jnp.bfloat16)
                width = vu.shape[2]
                heads_out[:, pl.ds(pl.multiple_of(h * width, width), width)] = value
            else:
                top[rows, :] = jnp.broadcast_to(highest, (T, 128))
                total[rows, :] = sums
                acc[rows, :] = summed
            return carry

        lax.fori_loop(begin, end, step, 0, unroll=8)

    def own_copy(zz):
        ref = rows_at(own_row, R)
        return pltpu.make_async_remote_copy(ref, ref, zs.at[zz], zr.at[z], z_dev(zz), MESH)

    def send_far(k):
        for n, d in enumerate((-1, 1)):
            def reach(n=n, d=d):
                pl.semaphore_wait(line_sem.at[n, k - 2], 1)
                if k < Z - 1:
                    pl.when(on_line(z + d))(partial(greet, line_sem.at[n, k - 1], z_dev(z + d)))
                own_copy(z - d * k).start()

            pl.when(on_line(z - d * k))(reach)

    greet(plane_sem, plane_devs[0])
    for n, d in enumerate((-1, 1)):
        pl.when(on_line(z + d) & on_line(z - d))(partial(greet, line_sem.at[n, 0], z_dev(z + d)))
    for d in (-1, 1):
        pl.when(on_line(z + d))(lambda d=d: own_copy(z + d).start())
    send_plane(0)
    token = lax.broadcasted_iota(jnp.int32, (T, 1), 0)
    query_places = jnp.zeros((T, 1), jnp.int32)
    for n in range(T // span_len):
        query_places = jnp.where(
            token // span_len == n, place_of(ctx * T + n * span_len) + lax.rem(token, span_len), query_places
        )
    cosine, sine = tables(query_places)
    first = lane < rope
    loads[2].wait()

    def turn(n, carry):
        values = qr[:, pl.ds(pl.multiple_of(n * 128, 128), 128)].astype(jnp.float32)
        value = rotate(values, cosine, sine) * scale
        row = pl.multiple_of(2 * n * T, T)
        queries[pl.ds(row, T), latent:] = jnp.where(first, value, 0.0).astype(jnp.bfloat16)
        queries[pl.ds(row + T, T), latent:] = jnp.where(first, 0.0, value).astype(jnp.bfloat16)
        return carry

    lax.fori_loop(0, H // 2, turn, 0)
    pl.semaphore_wait(plane_sem, 1)
    send(rows_at(own_row, R), ps.at[2, 0], pr.at[2, z], plane_devs[2])
    send_far(2)
    key_lane = lax.broadcasted_iota(jnp.int32, (1, L), 1)
    for n, plane in enumerate(planes):
        key_places = jnp.zeros((1, L), jnp.int32)
        for b in range(L // span_len):
            start = plane * L + b * span_len
            key_places = jnp.where(key_lane // span_len == b, place_of(start) + lax.rem(key_lane, span_len), key_places)
        bias[n] = jnp.where(key_places <= query_places, 0.0, fill_score)
    for k in range(3, Z):
        send_far(k)
    relay_plane(1)
    relay_sibling(0)
    loads[3].wait()
    loads[4].wait()

    def absorb(n, carry):
        value = jnp.dot(
            qp[:, pl.ds(pl.multiple_of(n * plain, plain), plain)], ku[n], preferred_element_type=jnp.float32
        )
        queries[pl.ds(pl.multiple_of(n * T, T), T), :latent] = (value * scale).astype(jnp.bfloat16)
        return carry

    lax.fori_loop(0, H, absorb, 0, unroll=4)

    for n in range(2, Z):
        relay_plane(n)
    relay_sibling(1)
    half = Z // 2
    for n in range(half):
        await_sibling(n)
        score(n)
    for n in range(half, Z):
        relay_sibling(n)
        part = H // (Z - half)
        attend(list(range(half)), True, False, (n - half) * part, (n - half + 1) * part)
    for n in range(half, Z):
        await_sibling(n)
        score(n)
    loads[5].wait()
    attend(list(range(half, Z)), False, True)
    loads[6].wait()

    def project(owner):
        return jnp.dot(
            heads_out[...], w[:, pl.ds(pl.multiple_of(owner * cols, 128), cols)],
            preferred_element_type=jnp.float32,
        )

    for j in (1, 0):
        target = lax.rem(y + j, Y) * C
        sib_out[j] = project(target + C - 1 - c).astype(jnp.bfloat16)
        copy = pltpu.make_async_remote_copy(sib_out.at[j], sib_in.at[j], rss.at[j], rsr.at[j], sibling, MESH)
        copy.start()
        own_part[...] = project(target + c)
        copy.wait_recv()
        sends.append(copy)
        if j > 0:
            y_out[...] = (own_part[...] + sib_in[j].astype(jnp.float32)).astype(jnp.bfloat16)
            y_copy = pltpu.make_async_remote_copy(y_out, y_in, rys.at[0], ryr.at[0], y_peer, MESH)
            y_copy.start()
            sends.append(y_copy)
    result = own_part[...] + sib_in[0].astype(jnp.float32)
    y_copy.wait_recv()
    out_ref[...] = (result + y_in[...].astype(jnp.float32)).astype(out_ref.dtype)
    for copy in sends:
        copy.wait_send()
    for n in range(1, Z):
        own_copy(planes[n]).wait_send()


def fused(dims, *arrays):
    Z, X, Y, C = dims
    query_plain, query_rotary, latent_keys, span_order, key_up, value_up, output_weight = arrays
    T = query_plain.shape[0]
    R = latent_keys.shape[0]
    H, plain, latent = key_up.shape
    tokens = R * Z * X * Y * C
    L = X * Y * C * R
    span_len = tokens // span_order.shape[0]
    cols = output_weight.shape[1] // (Y * C)
    bf16, f32 = jnp.bfloat16, jnp.float32
    dma = pltpu.SemaphoreType.DMA
    operands = (span_order, latent_keys, query_plain, query_rotary, key_up, value_up, output_weight)
    return pl.pallas_call(
        partial(fused_kernel, dims, span_len, latent),
        out_shape=pltpu.VMEM((T, cols), bf16),
        in_specs=[pl.BlockSpec(memory_space=pltpu.HBM)] * len(operands),
        out_specs=pl.BlockSpec(memory_space=pltpu.VMEM),
        scratch_shapes=[
            pltpu.SMEM(span_order.shape, jnp.int32),
            pltpu.VMEM(latent_keys.shape, bf16),
            pltpu.VMEM(query_plain.shape, bf16),
            pltpu.VMEM(query_rotary.shape, bf16),
            pltpu.VMEM(key_up.shape, bf16),
            pltpu.VMEM(value_up.shape, bf16),
            pltpu.VMEM(output_weight.shape, bf16),
            pltpu.VMEM((tokens, latent + 128), bf16),
            pltpu.VMEM((H * T, latent + 128), bf16),
            pltpu.VMEM((Z, T, L), f32),
            pltpu.VMEM((Z, H * T, L), f32),
            pltpu.VMEM((H * T, latent), f32),
            pltpu.VMEM((H * T, 128), f32),
            pltpu.VMEM((H * T, 128), f32),
            pltpu.VMEM((T, H * value_up.shape[2]), bf16),
            pltpu.VMEM((T, cols), f32),
            pltpu.VMEM((Y, T, cols), bf16),
            pltpu.VMEM((Y, T, cols), bf16),
            pltpu.VMEM((T, cols), bf16),
            pltpu.VMEM((T, cols), bf16),
            dma((7,)),
            pltpu.SemaphoreType.REGULAR, pltpu.SemaphoreType.REGULAR((2, Z - 2)),
            dma((Z,)), dma((Z,)),
            dma((3, Z)), dma((3, Z)),
            dma((Z, 4)), dma((Z, 4)),
            dma((Y,)), dma((Y,)),
            dma((1,)), dma((1,)),
        ],
        compiler_params=pltpu.CompilerParams(
            collective_id=0, has_side_effects=True, vmem_limit_bytes=56 * 1024 * 1024
        ),
    )(*(pltpu.with_memory_space_constraint(value, pltpu.HBM) for value in operands))


def chosen(mesh, *arrays):
    dims = split_axes(mesh)
    Z, X, Y, C = dims
    query_plain, query_rotary, latent_keys, span_order, key_up, value_up, output_weight = arrays
    R, T = latent_keys.shape[0], query_plain.shape[0]
    rope = latent_keys.shape[1] - key_up.shape[2]
    cols = output_weight.shape[1] // mesh.shape["tp"]
    fits = Z > 2 and X == Y == 2 and mesh.shape["tp"] == 4 and R % 16 == 0 and cols % 128 == 0
    fits = fits and rope * 2 == 128 and (X * Y * C * R) % 128 == 0 and key_up.shape[0] % 8 == 0 and key_up.shape[0] % (Z - Z // 2) == 0
    return fused(dims, *arrays) if fits else on_device(*arrays)


def solution(mesh):
    return jax.shard_map(
        partial(chosen, mesh),
        mesh=mesh,
        in_specs=(
            P("ctx", "tp"),
            P("ctx", "tp"),
            P(("ctx", "tp"), None),
            P(),
            P("tp", None, None),
            P("tp", None, None),
            P("tp", None),
        ),
        out_specs=P("ctx", "tp"),
        check_vma=False,
    )
```

```python
import math
from functools import partial

import jax
import jax.numpy as jnp
from jax import lax
from jax.experimental import pallas as pl
from jax.experimental.pallas import tpu as pltpu
from jax.sharding import PartitionSpec as P

rope_base = 10000.0
fill_score = -1e30
key_block_rows = 512


def rotate_pairs(values, places):
    halfway = values.shape[-1] // 2
    frequency = rope_base ** (-jnp.arange(halfway, dtype=jnp.float32) * 2.0 / values.shape[-1])
    angles = places.astype(jnp.float32)[:, None] * frequency[None, :]
    cosine = jnp.cos(angles)
    sine_part = jnp.sin(angles)
    if values.ndim == 3:
        cosine = cosine[:, None, :]
        sine_part = sine_part[:, None, :]
    first_half = values[..., :halfway]
    second_half = values[..., halfway:]
    return jnp.concatenate(
        [
            first_half * cosine - second_half * sine_part,
            first_half * sine_part + second_half * cosine,
        ],
        axis=-1,
    )


def token_places(span_table, indices, span_len):
    slot_ids = indices // span_len
    slot_table = jnp.arange(span_table.shape[0], dtype=jnp.int32)
    picked = jnp.sum(
        jnp.where(slot_ids[:, None] == slot_table[None, :], span_table[None, :], 0), axis=1
    )
    return picked * span_len + indices % span_len


def attend_block(
    carry_state, keys_block, key_places, queries, query_places, latent_width, score_scale
):
    running_max, running_sum, summed = carry_state
    scores = jnp.dot(queries, keys_block.T, preferred_element_type=jnp.float32) * score_scale
    allowed = key_places[None, :] <= query_places[:, None]
    masked = jnp.where(allowed, scores, fill_score)
    new_max = jnp.maximum(running_max, jnp.max(masked, axis=1))
    weights = jnp.where(allowed, jnp.exp(scores - new_max[:, None]), 0.0)
    factor = jnp.exp(running_max - new_max)
    new_sum = running_sum * factor + jnp.sum(weights, axis=1)
    new_summed = summed * factor[:, None] + jnp.dot(
        weights.astype(jnp.bfloat16),
        keys_block[:, :latent_width],
        preferred_element_type=jnp.float32,
    )
    return (new_max, new_sum, new_summed)


def attend_guarded(
    carry_state, keys_block, key_places, queries, query_places, latest, latent_width, score_scale
):
    return lax.cond(
        jnp.min(key_places) > latest,
        lambda carried: carried,
        lambda carried: attend_block(
            carried, keys_block, key_places, queries, query_places, latent_width, score_scale
        ),
        carry_state,
    )


def make_folder(queries, row_places, latest, span_order, span_len, latent_width, score_scale):

    def fold_piece(carry_state, key_piece, offset):
        piece_rows = key_piece.shape[0]
        key_places = token_places(span_order, jnp.arange(piece_rows, dtype=jnp.int32), span_len)

        def step_block(carried, block_parts):
            return (
                attend_guarded(
                    carried,
                    block_parts[0],
                    block_parts[1],
                    queries,
                    row_places,
                    latest,
                    latent_width,
                    score_scale,
                ),
                None,
            )

        stacked = key_piece.reshape(
            piece_rows // key_block_rows, key_block_rows, key_piece.shape[1]
        )
        stacked_places = key_places.reshape(piece_rows // key_block_rows, key_block_rows)
        result_state, unused = lax.scan(step_block, carry_state, (stacked, stacked_places))
        return result_state

    return fold_piece


def start_state(row_count, latent_width):
    return (
        jnp.full((row_count,), fill_score, jnp.float32),
        jnp.zeros((row_count,), jnp.float32),
        jnp.zeros((row_count,), jnp.float32)[:, None] + jnp.zeros((1, latent_width), jnp.float32),
    )


def project_out(final_state, token_count, head_count, latent_width, value_up, output_weight):
    running_max, running_sum, summed = final_state
    mixed_latent = (
        (summed / running_sum[:, None])
        .astype(jnp.bfloat16)
        .reshape(token_count, head_count, latent_width)
    )
    head_out = jnp.einsum(
        "thl,hlv->thv", mixed_latent, value_up, preferred_element_type=jnp.float32
    ).astype(jnp.bfloat16)
    head_out = head_out.reshape(token_count, head_count * value_up.shape[2])
    return jnp.dot(head_out, output_weight, preferred_element_type=jnp.float32)


def on_device(query_plain, query_rotary, latent_keys, span_order, key_up, value_up, output_weight):
    local_tokens = query_plain.shape[0]
    head_count = key_up.shape[0]
    plain_width = key_up.shape[1]
    latent_width = key_up.shape[2]
    rotary_width = query_rotary.shape[1] // head_count
    span_len = local_tokens // 2
    score_scale = 1.0 / math.sqrt(plain_width + rotary_width)
    first_row = lax.axis_index("ctx") * local_tokens
    query_places = token_places(
        span_order, first_row + jnp.arange(local_tokens, dtype=jnp.int32), span_len
    )
    absorbed = jnp.einsum(
        "thn,hnl->thl",
        query_plain.reshape(local_tokens, head_count, plain_width),
        key_up,
        preferred_element_type=jnp.float32,
    ).astype(jnp.bfloat16)
    turned = rotate_pairs(
        query_rotary.reshape(local_tokens, head_count, rotary_width).astype(jnp.float32),
        query_places,
    ).astype(jnp.bfloat16)
    queries = jnp.concatenate([absorbed, turned], axis=2).reshape(
        local_tokens * head_count, latent_width + rotary_width
    )
    row_places = jnp.repeat(query_places, head_count)
    own_rows = latent_keys.shape[0]
    own_first = first_row + lax.axis_index("tp") * own_rows
    own_places = token_places(
        span_order, own_first + jnp.arange(own_rows, dtype=jnp.int32), span_len
    )
    own_turned = rotate_pairs(latent_keys[:, latent_width:].astype(jnp.float32), own_places).astype(
        jnp.bfloat16
    )
    own_keys = jnp.concatenate([latent_keys[:, :latent_width], own_turned], axis=1)
    latest = jnp.max(query_places)
    folder = make_folder(
        queries, row_places, latest, span_order, span_len, latent_width, score_scale
    )
    group_keys = lax.all_gather(own_keys, "tp", axis=0, tiled=True)
    final_state = folder(
        start_state(local_tokens * head_count, latent_width),
        lax.all_gather(group_keys, "ctx", axis=0, tiled=True),
        jnp.int32(0),
    )
    head_terms = project_out(
        final_state, local_tokens, head_count, latent_width, value_up, output_weight
    )
    return lax.psum_scatter(head_terms.astype(jnp.bfloat16), "tp", scatter_dimension=1, tiled=True)


MESH = pl.DeviceIdType.MESH


def split_axes(mesh):
    ctx, tp = mesh.shape["ctx"], mesh.shape["tp"]
    x_size = 1
    while (2 * x_size) ** 2 <= ctx and ctx % (2 * x_size) == 0:
        x_size *= 2
    return ctx // x_size, x_size, tp // 2, 2


def fused_kernel(dims, span_len, latent, span_hbm, own_hbm, qp_hbm, qr_hbm, ku_hbm, vu_hbm, w_hbm,
                 out_ref, span_ref, own_ref, qp, qr, ku, vu, w, keys, queries, bias, scores, acc, top, total,
                 heads_out, own_part, sib_out, sib_in, y_out, y_in,
                 load_sem, plane_sem, line_sem, zs, zr, ps, pr, ss, sr, rss, rsr, rys, ryr):
    Z, X, Y, C = dims
    ctx = lax.axis_index("ctx")
    tp = lax.axis_index("tp")
    z, x = ctx // X, ctx % X
    y, c = tp // C, tp % C
    R = own_ref.shape[0]
    rope = own_ref.shape[1] - latent
    T = qp.shape[0]
    H, plain = ku.shape[0], ku.shape[1]
    L = X * Y * C * R
    cols = out_ref.shape[1]
    scale = math.log2(math.e) / math.sqrt(plain + rope)

    def z_dev(zz):
        return (zz * X + x, tp)

    sibling = (ctx, y * C + (C - 1 - c))
    y_peer = (ctx, (1 - y) * C + c)
    plane_devs = [(z * X + 1 - x, tp), y_peer, (z * X + 1 - x, (1 - y) * C + c)]

    def plane_cols(kind):
        return [(x, y), (1 - x, y), (x, 1 - y), (1 - x, 1 - y)][kind]

    def z_order(i):
        low = i + (i >= z).astype(jnp.int32)
        high = Z - 1 - i - (i >= Z - 1 - z).astype(jnp.int32)
        return jnp.where(z < Z // 2, low, high)

    planes = [z] + [z_order(jnp.int32(i)) for i in range(Z - 1)]

    barrier = pltpu.get_barrier_semaphore()

    def on_line(zz):
        return (zz >= 0) & (zz < Z)

    def greet(semaphore, device):
        pl.semaphore_signal(semaphore, inc=1, device_id=device, device_id_type=MESH)

    for peer in plane_devs[:2] + [sibling]:
        greet(barrier, peer)
    for d in (-1, 1):
        pl.when(on_line(z + d))(partial(greet, barrier, z_dev(z + d)))

    loads = []
    pairs = ((own_hbm, own_ref), (span_hbm, span_ref), (qr_hbm, qr), (qp_hbm, qp), (ku_hbm, ku), (vu_hbm, vu), (w_hbm, w))
    for n, (src, dst) in enumerate(pairs):
        load = pltpu.make_async_copy(src, dst, load_sem.at[n])
        load.start()
        loads.append(load)

    lane = lax.broadcasted_iota(jnp.int32, (1, 128), 1)
    pair = lax.rem(lane, rope // 2)
    frequency = jnp.zeros((1, 128), jnp.float32)
    for i in range(rope // 2):
        frequency = jnp.where(pair == i, rope_base ** (-2.0 * i / rope), frequency)
    low = lax.rem(lane, rope) < rope // 2

    def tables(places):
        angles = places.astype(jnp.float32) * frequency
        sine = jnp.sin(angles)
        return jnp.cos(angles), jnp.where(low, -sine, sine)

    def rotate(values, cosine, sine):
        swapped = jnp.where(
            low, pltpu.roll(values, 128 - rope // 2, 1), pltpu.roll(values, rope // 2, 1)
        )
        return values * cosine + swapped * sine

    def place_of(row):
        return span_ref[row // span_len] * span_len + lax.rem(row, span_len)

    loads[0].wait()
    loads[1].wait()
    own_row = ctx * T + tp * R
    own_places = place_of(own_row) + lax.broadcasted_iota(jnp.int32, (R, 1), 0)
    part = own_ref[:, latent:].astype(jnp.float32)
    turned = rotate(jnp.concatenate([part, part], axis=1), *tables(own_places)).astype(jnp.bfloat16)

    def block(zz, xx, yy, cc):
        return (((zz * X + xx) * Y + yy) * C + cc) * R

    def rows_at(start, size):
        return keys.at[pl.ds(pl.multiple_of(start, R), size)]

    mine = pl.ds(pl.multiple_of(own_row, R), R)
    keys[mine, :latent] = own_ref[:, :latent]
    keys[mine, latent:] = turned

    ends = on_line(z - 1).astype(jnp.int32) + on_line(z + 1).astype(jnp.int32)
    pl.semaphore_wait(barrier, 3 + ends)
    sends = []

    def send(ref, send_sem, recv_sem, device):
        copy = pltpu.make_async_remote_copy(ref, ref, send_sem, recv_sem, device, MESH)
        copy.start()
        sends.append(copy)

    def arrival(ref, send_sem, recv_sem, device):
        pltpu.make_async_remote_copy(ref, ref, send_sem, recv_sem, device, MESH).wait_recv()

    def send_sibling(n, kind):
        ref = rows_at(block(planes[n], *plane_cols(kind), c), R)
        send(ref, ss.at[n, kind], sr.at[n, kind], sibling)

    def send_plane(n):
        ref = rows_at(block(planes[n], x, y, c), R)
        for kind in (2, 0, 1) if n > 0 else (0, 1):
            send(ref, ps.at[kind, n], pr.at[kind, planes[n]], plane_devs[kind])
        send_sibling(n, 0)

    def relay_plane(n):
        zz = planes[n]
        arrival(rows_at(block(zz, x, y, c), R), zs.at[zz], zr.at[zz], z_dev(zz))
        send_plane(n)

    def relay_sibling(n):
        for kind in (0, 1, 2):
            ref = rows_at(block(planes[n], *plane_cols(kind + 1), c), R)
            arrival(ref, ps.at[kind, n], pr.at[kind, planes[n]], plane_devs[kind])
            send_sibling(n, kind + 1)

    def await_sibling(n):
        for kind in range(4):
            ref = rows_at(block(planes[n], *plane_cols(kind), C - 1 - c), R)
            arrival(ref, ss.at[n, kind], sr.at[n, kind], sibling)

    group = 8

    def plane_rows(n):
        return pl.ds(pl.multiple_of(planes[n] * L, L), L)

    def score(n):
        def step(m, carry):
            start = pl.multiple_of(m * (group * T), group * T)
            value = lax.dot_general(
                queries[pl.ds(start, group * T), :], keys[plane_rows(n), :],
                (((1,), (1,)), ((), ())), preferred_element_type=jnp.float32,
            )
            for g in range(group):
                scores[n, pl.ds(start + g * T, T), :] = value[g * T:(g + 1) * T] + bias[n]
            return carry

        lax.fori_loop(0, H // group, step, 0)

    def attend(members, opening, closing, begin=0, end=H):
        def step(h, carry):
            rows = pl.ds(pl.multiple_of(h * T, T), T)
            tiles = [scores[n, rows, k:k + 128] for n in members for k in range(0, L, 128)]
            highest = tiles[0]
            for tile in tiles[1:]:
                highest = jnp.maximum(highest, tile)
            highest = jnp.max(highest, axis=1, keepdims=True)
            if not opening:
                before = top[rows, :1]
                highest = jnp.maximum(highest, before)
                factor = jnp.exp2(before - highest)
            weights = []
            sums = None
            for tile in tiles:
                raised = jnp.exp2(tile - highest)
                sums = raised if sums is None else sums + raised
                weights.append(raised.astype(jnp.bfloat16))
            summed = None
            per = L // 128
            for i, n in enumerate(members):
                value = jnp.dot(
                    jnp.concatenate(weights[i * per:(i + 1) * per], axis=1), keys[plane_rows(n), :latent],
                    preferred_element_type=jnp.float32,
                )
                summed = value if summed is None else summed + value
            if not opening:
                sums = sums + total[rows, :] * factor
                summed = summed + acc[rows, :] * factor
            if closing:
                context = (summed * (1.0 / jnp.sum(sums, axis=1, keepdims=True))).astype(jnp.bfloat16)
                value = jnp.dot(context, vu[h], preferred_element_type=jnp.float32).astype(jnp.bfloat16)
                width = vu.shape[2]
                heads_out[:, pl.ds(pl.multiple_of(h * width, width), width)] = value
            else:
                top[rows, :] = jnp.broadcast_to(highest, (T, 128))
                total[rows, :] = sums
                acc[rows, :] = summed
            return carry

        lax.fori_loop(begin, end, step, 0, unroll=8)

    def own_copy(zz):
        ref = rows_at(own_row, R)
        return pltpu.make_async_remote_copy(ref, ref, zs.at[zz], zr.at[z], z_dev(zz), MESH)

    def send_far(k):
        for n, d in enumerate((-1, 1)):
            def reach(n=n, d=d):
                pl.semaphore_wait(line_sem.at[n, k - 2], 1)
                if k < Z - 1:
                    pl.when(on_line(z + d))(partial(greet, line_sem.at[n, k - 1], z_dev(z + d)))
                own_copy(z - d * k).start()

            pl.when(on_line(z - d * k))(reach)

    greet(plane_sem, plane_devs[0])
    for n, d in enumerate((-1, 1)):
        pl.when(on_line(z + d) & on_line(z - d))(partial(greet, line_sem.at[n, 0], z_dev(z + d)))
    for d in (-1, 1):
        pl.when(on_line(z + d))(lambda d=d: own_copy(z + d).start())
    send_plane(0)
    token = lax.broadcasted_iota(jnp.int32, (T, 1), 0)
    query_places = jnp.zeros((T, 1), jnp.int32)
    for n in range(T // span_len):
        query_places = jnp.where(
            token // span_len == n, place_of(ctx * T + n * span_len) + lax.rem(token, span_len), query_places
        )
    cosine, sine = tables(query_places)
    first = lane < rope
    loads[2].wait()

    def turn(n, carry):
        values = qr[:, pl.ds(pl.multiple_of(n * 128, 128), 128)].astype(jnp.float32)
        value = rotate(values, cosine, sine) * scale
        row = pl.multiple_of(2 * n * T, T)
        queries[pl.ds(row, T), latent:] = jnp.where(first, value, 0.0).astype(jnp.bfloat16)
        queries[pl.ds(row + T, T), latent:] = jnp.where(first, 0.0, value).astype(jnp.bfloat16)
        return carry

    lax.fori_loop(0, H // 2, turn, 0)
    pl.semaphore_wait(plane_sem, 1)
    send(rows_at(own_row, R), ps.at[2, 0], pr.at[2, z], plane_devs[2])
    send_far(2)
    key_lane = lax.broadcasted_iota(jnp.int32, (1, L), 1)
    for n, plane in enumerate(planes):
        key_places = jnp.zeros((1, L), jnp.int32)
        for b in range(L // span_len):
            start = plane * L + b * span_len
            key_places = jnp.where(key_lane // span_len == b, place_of(start) + lax.rem(key_lane, span_len), key_places)
        bias[n] = jnp.where(key_places <= query_places, 0.0, fill_score)
    for k in range(3, Z):
        send_far(k)
    relay_plane(1)
    relay_sibling(0)
    loads[3].wait()
    loads[4].wait()

    def absorb(n, carry):
        value = jnp.dot(
            qp[:, pl.ds(pl.multiple_of(n * plain, plain), plain)], ku[n], preferred_element_type=jnp.float32
        )
        queries[pl.ds(pl.multiple_of(n * T, T), T), :latent] = (value * scale).astype(jnp.bfloat16)
        return carry

    lax.fori_loop(0, H, absorb, 0, unroll=4)

    for n in range(2, Z):
        relay_plane(n)
    relay_sibling(1)
    half = Z // 2
    for n in range(half):
        await_sibling(n)
        score(n)
    for n in range(half, Z):
        relay_sibling(n)
        part = H // (Z - half)
        attend(list(range(half)), True, False, (n - half) * part, (n - half + 1) * part)
    for n in range(half, Z):
        await_sibling(n)
        score(n)
    loads[5].wait()
    attend(list(range(half, Z)), False, True)
    loads[6].wait()

    split = (cols // 256 + 1) // 2 * 256
    spans = ((0, split), (split, cols - split))

    def project(owner, begin, size):
        return jnp.dot(
            heads_out[...], w[:, pl.ds(pl.multiple_of(owner * cols + begin, 128), size)],
            preferred_element_type=jnp.float32,
        )

    def sibling_copy(j, n):
        part = pl.ds(spans[n][0], spans[n][1])
        return pltpu.make_async_remote_copy(
            sib_out.at[j, :, part], sib_in.at[j, :, part], rss.at[j, n], rsr.at[j, n], sibling, MESH
        )

    def peer_copy(n):
        part = pl.ds(spans[n][0], spans[n][1])
        return pltpu.make_async_remote_copy(y_out.at[:, part], y_in.at[:, part], rys.at[n], ryr.at[n], y_peer, MESH)

    for j in (1, 0):
        target = lax.rem(y + j, Y) * C
        for n, (begin, size) in enumerate(spans):
            sib_out[j, :, begin:begin + size] = project(target + C - 1 - c, begin, size).astype(jnp.bfloat16)
            copy = sibling_copy(j, n)
            copy.start()
            sends.append(copy)
        for n, (begin, size) in enumerate(spans):
            part = project(target + c, begin, size)
            if j > 0:
                sibling_copy(j, n).wait_recv()
                part = part + sib_in[j, :, begin:begin + size].astype(jnp.float32)
                y_out[:, begin:begin + size] = part.astype(jnp.bfloat16)
                copy = peer_copy(n)
                copy.start()
                sends.append(copy)
            else:
                own_part[:, begin:begin + size] = part
    for n, (begin, size) in enumerate(spans):
        sibling_copy(0, n).wait_recv()
        own_part[:, begin:begin + size] += sib_in[0, :, begin:begin + size].astype(jnp.float32)
    for n, (begin, size) in enumerate(spans):
        peer_copy(n).wait_recv()
        whole = own_part[:, begin:begin + size] + y_in[:, begin:begin + size].astype(jnp.float32)
        out_ref[:, begin:begin + size] = whole.astype(out_ref.dtype)
    for copy in sends:
        copy.wait_send()
    for n in range(1, Z):
        own_copy(planes[n]).wait_send()


def fused(dims, *arrays):
    Z, X, Y, C = dims
    query_plain, query_rotary, latent_keys, span_order, key_up, value_up, output_weight = arrays
    T = query_plain.shape[0]
    R = latent_keys.shape[0]
    H, plain, latent = key_up.shape
    tokens = R * Z * X * Y * C
    L = X * Y * C * R
    span_len = tokens // span_order.shape[0]
    cols = output_weight.shape[1] // (Y * C)
    bf16, f32 = jnp.bfloat16, jnp.float32
    dma = pltpu.SemaphoreType.DMA
    operands = (span_order, latent_keys, query_plain, query_rotary, key_up, value_up, output_weight)
    return pl.pallas_call(
        partial(fused_kernel, dims, span_len, latent),
        out_shape=pltpu.VMEM((T, cols), bf16),
        in_specs=[pl.BlockSpec(memory_space=pltpu.HBM)] * len(operands),
        out_specs=pl.BlockSpec(memory_space=pltpu.VMEM),
        scratch_shapes=[
            pltpu.SMEM(span_order.shape, jnp.int32),
            pltpu.VMEM(latent_keys.shape, bf16),
            pltpu.VMEM(query_plain.shape, bf16),
            pltpu.VMEM(query_rotary.shape, bf16),
            pltpu.VMEM(key_up.shape, bf16),
            pltpu.VMEM(value_up.shape, bf16),
            pltpu.VMEM(output_weight.shape, bf16),
            pltpu.VMEM((tokens, latent + 128), bf16),
            pltpu.VMEM((H * T, latent + 128), bf16),
            pltpu.VMEM((Z, T, L), f32),
            pltpu.VMEM((Z, H * T, L), f32),
            pltpu.VMEM((H * T, latent), f32),
            pltpu.VMEM((H * T, 128), f32),
            pltpu.VMEM((H * T, 128), f32),
            pltpu.VMEM((T, H * value_up.shape[2]), bf16),
            pltpu.VMEM((T, cols), f32),
            pltpu.VMEM((Y, T, cols), bf16),
            pltpu.VMEM((Y, T, cols), bf16),
            pltpu.VMEM((T, cols), bf16),
            pltpu.VMEM((T, cols), bf16),
            dma((7,)),
            pltpu.SemaphoreType.REGULAR, pltpu.SemaphoreType.REGULAR((2, Z - 2)),
            dma((Z,)), dma((Z,)),
            dma((3, Z)), dma((3, Z)),
            dma((Z, 4)), dma((Z, 4)),
            dma((Y, 2)), dma((Y, 2)),
            dma((2,)), dma((2,)),
        ],
        compiler_params=pltpu.CompilerParams(
            collective_id=0, has_side_effects=True, vmem_limit_bytes=56 * 1024 * 1024
        ),
    )(*(pltpu.with_memory_space_constraint(value, pltpu.HBM) for value in operands))


def chosen(mesh, *arrays):
    dims = split_axes(mesh)
    Z, X, Y, C = dims
    query_plain, query_rotary, latent_keys, span_order, key_up, value_up, output_weight = arrays
    R, T = latent_keys.shape[0], query_plain.shape[0]
    rope = latent_keys.shape[1] - key_up.shape[2]
    cols = output_weight.shape[1] // mesh.shape["tp"]
    fits = Z > 2 and X == Y == 2 and mesh.shape["tp"] == 4 and R % 16 == 0 and cols % 128 == 0 and cols > 256
    fits = fits and rope * 2 == 128 and (X * Y * C * R) % 128 == 0 and key_up.shape[0] % 8 == 0 and key_up.shape[0] % (Z - Z // 2) == 0
    return fused(dims, *arrays) if fits else on_device(*arrays)


def solution(mesh):
    return jax.shard_map(
        partial(chosen, mesh),
        mesh=mesh,
        in_specs=(
            P("ctx", "tp"),
            P("ctx", "tp"),
            P(("ctx", "tp"), None),
            P(),
            P("tp", None, None),
            P("tp", None, None),
            P("tp", None),
        ),
        out_specs=P("ctx", "tp"),
        check_vma=False,
    )
```
